32 devices in a mesh: samp: 4 (over z), row: 2 (over y), col: 4 (over x, core).
Axes of the slice: x: 2, y: 2, z: 4, core: 2. Of those that a mesh axis runs over, the one named last changes fastest.
Arguments:
- tokens: bfloat16 [4, 256, 768], P('samp', 'row'), may hold values from -6 to 6
- atom_type: int32 [256], P('row'), may hold values from 0 to 31
- noise_step: int32 [4], P('samp'), may hold values from 0 to 199
- pair_rep: bfloat16 [256, 256, 128], P('row', 'col'), may hold values from -8 to 8
- bond_blocks: int32 [64, 2], replicated, may hold values from 0 to 7
- chiral_blocks: int32 [32, 2], replicated, may hold values from 0 to 7
- type_table: bfloat16 [32, 768], replicated, may hold values from -6 to 6
- noise_row: float32 [768], replicated, may hold values from -6 to 6
- norm_gain: float32 [768], replicated, may hold values from 0.5 to 1.5
- pair_gain: float32 [128], replicated, may hold values from 0.5 to 1.5
- in_weight: bfloat16 [4, 768, 768], P(None, 'col'), may hold values from -0.21875 to 0.21875
- out_weight: bfloat16 [768, 768], P('col'), may hold values from -0.21875 to 0.21875
- pair_weight: float32 [128, 16], replicated, may hold values from -16 to 16
- restraint_weight: float32 [2, 16], replicated, may hold values from -3 to 3
- cotangent: bfloat16 [4, 256, 768], P('samp', 'row'), may hold values from -6 to 6
Outputs:
- updated: bfloat16 [4, 256, 768], P('samp', 'row')
- token_grad: bfloat16 [4, 256, 768], P('samp', 'row')
- pair_grad: bfloat16 [256, 256, 128], P('row', 'col', 'samp')
- in_grad: bfloat16 [4, 768, 768], P(None, 'col')
- out_grad: bfloat16 [768, 768], P('col')
- proj_grad: float32 [128, 16], replicated
The draws below stay inside these ranges and needn't reach their ends.
All inputs are finite; a program needn't handle non-finite values.
Results may differ from the reference program's by a relative error of at most 0.015.
Values may be sent and summed in bfloat16 or wider, within the bound.
No kernel may reach another device: no remote copies, remote signals or barrier semaphores. Data moves between devices by JAX's collectives and lax.ppermute only.
A program may use at most 128 MiB of HBM per device.

```python
import math
import jax
import jax.numpy as jnp
import numpy as np
from jax import lax

D = 768
HEADS = 16
HEAD_DIM = 48
PAIR_CH = 128
TYPES = 32
BONDS = 64
CHIRAL = 32
BLOCK = 32
STEPS = 200
TOKENS = 256
SAMPLES = 4


def draw_pair_rep(key, part):
    array_shape = (TOKENS, TOKENS, PAIR_CH)
    key_values = jax.random.fold_in(jax.random.fold_in(key, 11), 1)
    entries = jax.random.normal(key_values, array_shape, jnp.float32)
    return jnp.clip(entries, -8.0, 8.0).astype(jnp.bfloat16)


def draw_pair_weight(key, part):
    key_values = jax.random.fold_in(jax.random.fold_in(key, 23), 0)
    entries = jax.random.normal(key_values, (PAIR_CH, HEADS), jnp.float32) * PAIR_CH ** (-0.5)
    return jnp.clip(entries, -16.0, 16.0)


def set_ends(array, own_key, least, high):
    spot = [jax.random.randint(jax.random.fold_in(own_key, axis), (), 0, length) for axis, length in enumerate(array.shape)]
    main_axis = array.shape.index(max(array.shape))
    next_to = spot[:main_axis] + [(spot[main_axis] + 1) % array.shape[main_axis]] + spot[main_axis + 1:]
    return array.at[tuple(spot)].set(least).at[tuple(next_to)].set(high)


def block_scale(own_key, dims, shards, least, largest):
    def one(dim, shards_of):
        draws = jax.random.uniform(jax.random.fold_in(jax.random.fold_in(own_key, 6), dim), (shards_of,), jnp.float32, least / len(shards), largest / len(shards))
        return jnp.repeat(jnp.exp(draws), dims[dim] // shards_of).reshape((-1,) + (1,) * (len(dims) - dim - 1))

    factor_of = one(*shards[0])
    for cut in shards[1:]:
        factor_of = factor_of * one(*cut)
    return factor_of


def rank_table(count, skew):
    loads = [(1 << 20) // math.isqrt(rank ** skew) + 1 for rank in range(1, count + 1)]
    scale = 1 + sum(loads) // (1 << 30)
    return np.cumsum(np.array([max(1, weight // scale) for weight in loads]))


def ranked(key, shape, number_of, skew):
    listing = rank_table(number_of, skew)
    ticket = jax.random.randint(jax.random.fold_in(key, 1), shape, 0, int(listing[number_of - 1]))
    grade = jnp.searchsorted(jnp.asarray(listing, jnp.int32), ticket, side="right")
    return jax.random.permutation(jax.random.fold_in(key, 2), number_of)[grade].astype(jnp.int32)


def scatter_about(own_key, dims, scale, bound, shards=(), kind=jnp.bfloat16):
    values = jax.random.normal(own_key, dims, jnp.float32) * scale
    if len(shards) > 0:
        values = block_scale(own_key, dims, shards, -0.22, 0.18) * values
    return jnp.clip(values, min=-bound, max=bound).astype(kind)


def setup_inputs(seed: int = 0) -> dict:
    streams_of = jax.random.split(jax.random.key(seed), 16)
    return {
        "tokens": scatter_about(streams_of[0], (SAMPLES, TOKENS, D), 1.0, 6.0, ((0, 4), (1, 2))),
        "atom_type": set_ends(ranked(streams_of[1], (TOKENS,), TYPES, 2), jax.random.fold_in(streams_of[1], 3), 0, TYPES - 1).astype(jnp.int32),
        "noise_step": set_ends(jax.random.randint(streams_of[2], (SAMPLES,), 0, STEPS), jax.random.fold_in(streams_of[2], 1), 0, STEPS - 1).astype(jnp.int32),
        "pair_rep": draw_pair_rep(jax.random.fold_in(streams_of[15], 71), 0),
        "bond_blocks": set_ends(jax.random.randint(streams_of[4], (BONDS, 2), 0, TOKENS // BLOCK), jax.random.fold_in(streams_of[4], 1), 0, (TOKENS // BLOCK) - 1).astype(jnp.int32),
        "chiral_blocks": set_ends(jax.random.randint(streams_of[5], (CHIRAL, 2), 0, TOKENS // BLOCK), jax.random.fold_in(streams_of[5], 1), 0, (TOKENS // BLOCK) - 1).astype(jnp.int32),
        "type_table": scatter_about(streams_of[6], (TYPES, D), 1.0, 6.0),
        "noise_row": scatter_about(streams_of[7], (D,), 1.0, 6.0, (), jnp.float32),
        "norm_gain": jnp.clip(1.0 + 0.1 * jax.random.normal(streams_of[8], (D,), jnp.float32), 0.5, 1.5),
        "pair_gain": jnp.clip(1.0 + 0.1 * jax.random.normal(streams_of[9], (PAIR_CH,), jnp.float32), 0.5, 1.5),
        "in_weight": scatter_about(streams_of[10], (4, HEADS * HEAD_DIM, D), D ** -0.5, 0.21875, ((1, 4),)),
        "out_weight": scatter_about(streams_of[11], (HEADS * HEAD_DIM, D), (HEADS * HEAD_DIM) ** -0.5, 0.21875, ((0, 4),)),
        "pair_weight": draw_pair_weight(jax.random.fold_in(streams_of[15], 71), 0),
        "restraint_weight": jnp.clip(jax.random.uniform(streams_of[13], (2, HEADS), jnp.float32, -3.0, 3.0), -3.0, 3.0),
        "cotangent": scatter_about(streams_of[14], (SAMPLES, TOKENS, D), 1.0, 6.0, ((0, 4), (1, 2))),
    }


eps = 1e-05

def rounded(values):
    return lax.optimization_barrier(values.astype(jnp.bfloat16)).astype(jnp.float32)

def noise_level(noise_step):
    top_root = 160.0 ** (1.0 / 7.0)
    low_root = 0.0004 ** (1.0 / 7.0)
    root_base = top_root + noise_step.astype(jnp.float32) / (STEPS - 1) * (low_root - top_root)
    return 7.0 / 4.0 * jnp.log(root_base)

def normalize(values, scales):
    center = lax.optimization_barrier(jnp.mean(values, axis=-1, keepdims=True))
    centered = values - center
    inv_std = lax.rsqrt(lax.optimization_barrier(jnp.mean(centered * centered, axis=-1, keepdims=True)) + eps)
    unit_rows = centered * inv_std
    return (unit_rows, inv_std, unit_rows * scales)

def norm_back(upstream, unit_rows, inv_std, scales):
    scaled = upstream * scales
    return inv_std * (scaled - lax.optimization_barrier(jnp.mean(scaled, axis=-1, keepdims=True)) - unit_rows * lax.optimization_barrier(jnp.mean(scaled * unit_rows, axis=-1, keepdims=True)))

def restraint_map(blocks, row_first, row_total, col_first, col_total, block_total):
    first_hot = jax.nn.one_hot(blocks[:, 0], block_total, dtype=jnp.float32)
    second_hot = jax.nn.one_hot(blocks[:, 1], block_total, dtype=jnp.float32)
    counts = jnp.dot(first_hot.T, second_hot)
    row_hot = jax.nn.one_hot((row_first + jnp.arange(row_total)) // BLOCK, block_total, dtype=jnp.float32)
    col_hot = jax.nn.one_hot((col_first + jnp.arange(col_total)) // BLOCK, block_total, dtype=jnp.float32)
    return jnp.dot(jnp.dot(row_hot, counts), col_hot.T)

def sample_pass(base_one, cot_one, bias_full, norm_gain, in_weight, out_weight):
    highest = lax.Precision.HIGHEST
    unit_rows, inv_std, token_scaled = normalize(base_one, norm_gain)
    normed = token_scaled.astype(jnp.bfloat16)
    projected = jnp.einsum('nd,mkd->nmk', normed.astype(jnp.float32), in_weight.astype(jnp.float32), precision=highest)
    query_heads = rounded(projected[:, 0]).reshape(TOKENS, HEADS, HEAD_DIM)
    key_heads = rounded(projected[:, 1]).reshape(TOKENS, HEADS, HEAD_DIM)
    value_heads = rounded(projected[:, 2]).reshape(TOKENS, HEADS, HEAD_DIM)
    gate_value = jax.nn.sigmoid(projected[:, 3])
    score_scale = 1.0 / math.sqrt(HEAD_DIM)
    scores = jnp.einsum('qhd,khd->hqk', query_heads, key_heads) * score_scale + bias_full
    attn_probs = jax.nn.softmax(scores, axis=-1)
    attn_low = rounded(attn_probs)
    attended = jnp.einsum('hqk,khd->qhd', attn_low, value_heads).reshape(TOKENS, -1)
    mixed = (gate_value * attended).astype(jnp.bfloat16)
    updated_one = (base_one + jnp.dot(mixed, out_weight, preferred_element_type=jnp.float32)).astype(jnp.bfloat16)
    out_one = jnp.dot(mixed.T, cot_one, preferred_element_type=jnp.float32)
    grad_mixed = jnp.dot(cot_one, out_weight.T, preferred_element_type=jnp.float32)
    attend_heads = rounded(grad_mixed * gate_value).reshape(TOKENS, HEADS, HEAD_DIM)
    grad_gate = grad_mixed * attended * gate_value * (1.0 - gate_value)
    grad_probs = jnp.einsum('qhd,khd->hqk', attend_heads, value_heads)
    row_delta = lax.optimization_barrier(jnp.sum(attn_probs * grad_probs, axis=-1, keepdims=True))
    grad_scores = attn_probs * (grad_probs - row_delta)
    grad_low = rounded(grad_scores)
    grad_query = jnp.einsum('hqk,khd->qhd', grad_low, key_heads).reshape(TOKENS, -1) * score_scale
    grad_keys = jnp.einsum('hqk,qhd->khd', grad_low, query_heads).reshape(TOKENS, -1) * score_scale
    grad_values = jnp.einsum('hqk,qhd->khd', attn_low, attend_heads).reshape(TOKENS, -1)
    grads = jnp.stack([grad_query, grad_keys, grad_values, grad_gate], axis=1)
    in_one = jnp.einsum('nd,nmk->mkd', normed.astype(jnp.float32), grads, precision=highest)
    grad_normed = jnp.einsum('nmk,mkd->nd', grads, in_weight.astype(jnp.float32), precision=highest)
    token_one = (cot_one.astype(jnp.float32) + norm_back(grad_normed, unit_rows, inv_std, norm_gain)).astype(jnp.bfloat16)
    return (updated_one, token_one, grad_scores, in_one, out_one)

def reference(tokens, atom_type, noise_step, pair_rep, bond_blocks, chiral_blocks, type_table, noise_row, norm_gain, pair_gain, in_weight, out_weight, pair_weight, restraint_weight, cotangent):
    highest = lax.Precision.HIGHEST
    block_total = TOKENS // BLOCK
    unit_pair, pair_inv, pair_scaled = normalize(pair_rep.astype(jnp.float32), pair_gain)
    bond_map = restraint_map(bond_blocks, 0, TOKENS, 0, TOKENS, block_total)
    chiral_map = restraint_map(chiral_blocks, 0, TOKENS, 0, TOKENS, block_total)
    bias_full = jnp.einsum('ijc,ch->hij', pair_scaled, pair_weight, precision=highest)
    bias_full = bias_full + restraint_weight[0][:, None, None] * bond_map + restraint_weight[1][:, None, None] * chiral_map
    type_rows = jnp.dot(jax.nn.one_hot(atom_type, TYPES, dtype=jnp.bfloat16), type_table, preferred_element_type=jnp.float32)
    noise_levels = noise_level(noise_step)
    base_rows = tokens.astype(jnp.float32) + type_rows[None] + noise_levels[:, None, None] * noise_row

    def one_sample(carry, inputs):
        base_one, cot_one = inputs
        updated_one, token_one, bias_one, in_one, out_one = sample_pass(base_one, cot_one, bias_full, norm_gain, in_weight, out_weight)
        bias_acc, in_acc, out_acc = carry
        return ((bias_acc + bias_one, in_acc + in_one, out_acc + out_one), (updated_one, token_one))
    start_carry = (jnp.zeros((HEADS, TOKENS, TOKENS), jnp.float32), jnp.zeros(in_weight.shape, jnp.float32), jnp.zeros(out_weight.shape, jnp.float32))
    (bias_grad, in_grad, out_grad), (updated, token_grad) = lax.scan(one_sample, start_carry, (base_rows, cotangent))
    spread = jnp.einsum('hij,ch->ijc', bias_grad, pair_weight, precision=highest)
    pair_grad = norm_back(spread, unit_pair, pair_inv, pair_gain).astype(jnp.bfloat16)
    proj_grad = jnp.einsum('ijc,hij->ch', pair_scaled, bias_grad, precision=highest)
    return (updated, token_grad, pair_grad, in_grad.astype(jnp.bfloat16), out_grad.astype(jnp.bfloat16), proj_grad)
```

```python
import functools
import math

import jax
import jax.numpy as jnp
from jax import lax
from jax.experimental import pallas as pl
from jax.experimental.pallas import tpu as pltpu
from jax.sharding import PartitionSpec as P


HEAD_DIM = 48
BLOCK = 32
STEPS = 200
EPS = 1e-05
BF = jnp.bfloat16
F32 = jnp.float32
HIGHEST = lax.Precision.HIGHEST

UNROLL = 4


def dot(left, right, left_dim, right_dim, precision=None):
    return lax.dot_general(
        left,
        right,
        (((left_dim,), (right_dim,)), ((), ())),
        precision=precision,
        preferred_element_type=F32,
    )


def split3(values):
    high = values.astype(BF)
    rest = values - high.astype(F32)
    middle = rest.astype(BF)
    low = (rest - middle.astype(F32)).astype(BF)
    return high, middle, low


def head_shift(first, heads):
    row = lax.broadcasted_iota(jnp.int32, (heads, heads), 0)
    column = lax.broadcasted_iota(jnp.int32, (heads, heads), 1)
    return (column == lax.rem(row + first, heads)).astype(F32)


class Spot:
    def __init__(self, index_ref, sizes):
        _, row, col = sizes
        flat = index_ref[0]
        self.col = lax.rem(flat, col)
        self.row = lax.rem(lax.div(flat, col), row)
        self.samp = lax.div(flat, col * row)


def pair_body(sizes, index_ref, pair_ref, gain_ref, weight_ref, *refs):
    _, _, col = sizes
    planes = refs[:col]
    unit_ref, inv_ref, flat = refs[col:]
    spot = Spot(index_ref, sizes)
    heads, channels = weight_ref.shape
    keys, rows = inv_ref.shape
    head_local = heads // col
    step = 512

    def widen(k, carry):
        part = pl.ds(pl.multiple_of(k * step, step), step)
        flat[part, :] = pair_ref[part, :].astype(F32)
        return carry

    lax.fori_loop(0, keys * rows // step, widen, 0)
    picked = dot(head_shift(spot.col * head_local, heads), weight_ref[...], 1, 0, HIGHEST)
    scaled = picked * gain_ref[...]
    high, middle, low = split3(scaled)
    total = jnp.sum(scaled, axis=1, keepdims=True)
    row_id = lax.broadcasted_iota(jnp.int32, (channels, channels), 0)
    column_id = lax.broadcasted_iota(jnp.int32, (channels, channels), 1)
    same = (row_id == column_id).astype(F32).astype(BF)
    left = jnp.concatenate([same, high, middle, low], axis=0)

    def one(j, carry):
        block = flat[pl.ds(j, rows, stride=keys), :].astype(BF)
        both = dot(left, block, 1, 1)
        values = both[:channels]
        mapped = (
            both[channels : channels + heads]
            + both[channels + heads : channels + 2 * heads]
            + both[channels + 2 * heads :]
        )
        mean = jnp.sum(values, axis=0, keepdims=True) * (1.0 / channels)
        centered = values - mean
        inv = lax.rsqrt(jnp.sum(centered * centered, axis=0, keepdims=True) * (1.0 / channels) + EPS)
        plane = (mapped - total * mean) * inv
        for k in range(col):
            planes[k][pl.ds(j, head_local, stride=keys), :] = plane[
                k * head_local : (k + 1) * head_local
            ]
        unit_ref[j] = (centered * inv).astype(BF)
        inv_ref[pl.ds(j, 1), :] = inv
        return carry

    lax.fori_loop(0, keys, one, 0, unroll=UNROLL)


def lanes(ref):
    return jnp.concatenate([ref[k : k + 1] for k in range(ref.shape[0])], axis=1)


def token_body(
    sizes,
    index_ref,
    step_ref,
    token_ref,
    type_ref,
    table_ref,
    noise_ref,
    gain_ref,
    in_ref,
    out_ref,
    cot_ref,
    after_ref,
    query_ref,
    key_value_ref,
    gates_ref,
    piece_ref,
    base_ref,
    normed_all,
):
    _, _, col = sizes
    spot = Spot(index_ref, sizes)
    rows, width = token_ref.shape
    types = table_ref.shape[0]
    kind = lax.broadcasted_iota(jnp.int32, (types, rows), 0) == type_ref[...]
    type_rows = dot(kind.astype(F32).astype(BF), table_ref[...], 0, 0)
    top_root = 160.0 ** (1.0 / 7.0)
    low_root = 0.0004 ** (1.0 / 7.0)
    count = jnp.full((1, width), step_ref[0], jnp.int32).astype(F32)
    level = 7.0 / 4.0 * jnp.log(top_root + count / (STEPS - 1) * (low_root - top_root))
    base = token_ref[...].astype(F32) + type_rows + level * lanes(noise_ref)
    base_ref[...] = base
    center = jnp.mean(base, axis=1, keepdims=True)
    centered = base - center
    inv = lax.rsqrt(jnp.mean(centered * centered, axis=1, keepdims=True) + EPS)
    normed = (centered * inv * lanes(gain_ref)).astype(BF)
    normed_all[...] = normed
    slab = rows // col
    part = pl.ds(pl.multiple_of(spot.col * slab, slab), slab)
    piece_ref[:, :width] = normed_all[part, :]
    piece_ref[:, width:] = cot_ref[part, :]
    inner = in_ref.shape[1]
    query_ref[...] = dot(in_ref[0], normed, 1, 1).astype(BF)
    key_value_ref[:inner] = dot(in_ref[1], normed, 1, 1).astype(BF)
    key_value_ref[inner:] = dot(in_ref[2], normed, 1, 1).astype(BF)
    gates_ref[:inner] = jax.nn.sigmoid(dot(in_ref[3], normed, 1, 1))
    gates_ref[inner:] = dot(out_ref[...], cot_ref[...], 1, 1)


def attention_body(sizes, head_local, index_ref, rest_ref, bond_ref, chiral_ref, query_ref, gates_ref, *refs):
    _, row, col = sizes
    key_values = refs[:row]
    planes = refs[row : row + col]
    refs = refs[row + col :]
    mixed_ref, grads_ref, own_ref = refs[:3]
    sends = refs[3 : 2 + row]
    bias_out = refs[2 + row : 2 + row + col]
    keys_all, values_all, bias, grad_kv, grad_bias = refs[2 + row + col :]
    spot = Spot(index_ref, sizes)
    inner, rows = query_ref.shape
    tokens = rows * row
    cols = tokens // col

    for t in range(row):
        part = pl.ds(pl.multiple_of(lax.rem(spot.row - t + row, row) * rows, rows), rows)
        keys_all[:, part] = key_values[t][:inner]
        values_all[:, part] = key_values[t][inner:]
    for k in range(col):
        first = lax.rem(spot.col - k + col, col) * cols
        for h in range(head_local):
            bias[pl.ds(pl.multiple_of(h * tokens + first, cols), cols), :] = planes[k][
                h * cols : (h + 1) * cols
            ]

    def counts(blocks_ref):
        blocks = blocks_ref.shape[1]
        key_block = lax.broadcasted_iota(jnp.int32, (tokens, blocks), 0) // BLOCK
        row_block = (lax.broadcasted_iota(jnp.int32, (rows, blocks), 0) + spot.row * rows) // BLOCK
        second = (blocks_ref[1:2] == key_block).astype(F32).astype(BF)
        first = (blocks_ref[0:1] == row_block).astype(F32).astype(BF)
        return dot(second, first, 1, 1)

    bond_map = counts(bond_ref)
    chiral_map = counts(chiral_ref)
    scale = 1.0 / math.sqrt(HEAD_DIM)
    for h in range(head_local):
        own = slice(h * HEAD_DIM, (h + 1) * HEAD_DIM)
        low = slice(inner + h * HEAD_DIM, inner + (h + 1) * HEAD_DIM)
        head = spot.col * head_local + h
        key, value, query = keys_all[own], values_all[own], query_ref[own]
        bias_h = (
            bias[h * tokens : (h + 1) * tokens]
            + rest_ref[0, head] * bond_map
            + rest_ref[1, head] * chiral_map
        )
        scores = dot(key, query, 0, 0) * scale + bias_h
        powers = jnp.exp(scores - jnp.max(scores, axis=0, keepdims=True))
        probs = powers * (1.0 / jnp.sum(powers, axis=0, keepdims=True))
        probs_low = probs.astype(BF)
        attended = dot(value, probs_low, 1, 0)
        gate, grad_mixed = gates_ref[own], gates_ref[low]
        mixed_ref[own] = (gate * attended).astype(BF)
        grad_attend = (grad_mixed * gate).astype(BF)
        grads_ref[low] = grad_mixed * attended * gate * (1.0 - gate)
        grad_probs = dot(value, grad_attend, 0, 0)
        delta = jnp.sum(probs * grad_probs, axis=0, keepdims=True)
        grad_scores = probs * (grad_probs - delta)
        grad_low = grad_scores.astype(BF)
        grad_bias[h * tokens : (h + 1) * tokens] = grad_low
        grads_ref[own] = dot(key, grad_low, 1, 0) * scale
        grad_kv[own] = dot(query, grad_low, 1, 1) * scale
        grad_kv[low] = dot(grad_attend, probs_low, 1, 1)
    own_ref[...] = grad_kv[:, pl.ds(pl.multiple_of(spot.row * rows, rows), rows)]
    for t in range(1, row):
        part = pl.ds(pl.multiple_of(lax.rem(spot.row + t, row) * rows, rows), rows)
        sends[t - 1][...] = grad_kv[:, part].astype(BF)
    for k in range(col):
        first = lax.rem(spot.col - k + col, col) * cols
        for h in range(head_local):
            bias_out[k][h * cols : (h + 1) * cols] = grad_bias[
                pl.ds(pl.multiple_of(h * tokens + first, cols), cols), :
            ]


def back_body(sizes, grads_ref, own_ref, mixed_ref, in_ref, out_ref, *refs):
    _, row, _ = sizes
    received = refs[: row - 1]
    factor_ref, both_ref = refs[row - 1 :]
    inner, rows = mixed_ref.shape
    key_value = own_ref[...]
    for other in received:
        key_value = key_value + other[...].astype(F32)
    grads = jnp.concatenate([grads_ref[:inner], key_value, grads_ref[inner:]], axis=0)
    high = grads.astype(BF)
    low = (grads - high.astype(F32)).astype(BF)
    factor_ref[:inner] = mixed_ref[...]
    factor_ref[inner:] = high
    both_ref[:rows] = dot(mixed_ref[...], out_ref[...], 0, 0).astype(BF)
    both_ref[rows:] = (dot(high, in_ref[...], 0, 0) + dot(low, in_ref[...], 0, 0)).astype(BF)


def finish_body(base_ref, cot_ref, gain_ref, first_ref, second_ref, updated_ref, grad_ref):
    rows = base_ref.shape[0]
    total = first_ref[...].astype(F32) + second_ref[...].astype(F32)
    base = base_ref[...]
    updated_ref[...] = (base + total[:rows]).astype(BF)
    center = jnp.mean(base, axis=1, keepdims=True)
    centered = base - center
    inv = lax.rsqrt(jnp.mean(centered * centered, axis=1, keepdims=True) + EPS)
    unit = centered * inv
    scaled = total[rows:] * lanes(gain_ref)
    grad = inv * (
        scaled
        - jnp.mean(scaled, axis=1, keepdims=True)
        - unit * jnp.mean(scaled * unit, axis=1, keepdims=True)
    )
    grad_ref[...] = (cot_ref[...].astype(F32) + grad).astype(BF)


def proj_body(sizes, index_ref, unit_ref, gain_ref, bias_ref, proj_ref, wide):
    col = sizes[2]
    spot = Spot(index_ref, sizes)
    keys, channels, _ = unit_ref.shape
    heads = bias_ref.shape[0] // keys
    wide[...] = bias_ref[...].astype(F32)

    def one(j, total):
        return total + dot(wide[pl.ds(j, heads, stride=keys), :].astype(BF), unit_ref[j], 1, 1)

    total = lax.fori_loop(0, keys, one, jnp.zeros((heads, channels), F32), unroll=8)
    total = dot(head_shift(spot.col * (heads // col), heads), total, 0, 0, HIGHEST)
    proj_ref[...] = total * gain_ref[...]


def pair_back_body(sizes, index_ref, unit_ref, inv_ref, weight_ref, gain_ref, first_ref, second_ref, *refs):
    samp, _, col = sizes
    planes = refs[:col]
    out_ref, wide = refs[col:]
    spot = Spot(index_ref, sizes)
    keys, channels, _ = unit_ref.shape
    own = channels // samp
    heads = weight_ref.shape[0]
    head_local = heads // col
    picked = dot(head_shift(spot.col * head_local, heads), weight_ref[...], 1, 0, HIGHEST)
    scaled = picked * gain_ref[...]
    scaled = scaled - jnp.mean(scaled, axis=1, keepdims=True)
    row_id = lax.broadcasted_iota(jnp.int32, (own, channels), 0)
    column_id = lax.broadcasted_iota(jnp.int32, (own, channels), 1)
    picks = (column_id == row_id + spot.samp * own).astype(F32)
    left = jnp.concatenate(split3(dot(picks, scaled, 1, 1, HIGHEST)), axis=1)
    wide[...] = first_ref[...].astype(F32) + second_ref[...].astype(F32)
    part = pl.ds(pl.multiple_of(spot.samp * own, own), own)

    def one(j, carry):
        grad = wide[pl.ds(j, heads, stride=keys), :]
        plane = jnp.concatenate(
            [planes[k][pl.ds(j, head_local, stride=keys), :] for k in range(col)], axis=0
        )
        joint = jnp.sum(grad * plane, axis=0, keepdims=True) * (1.0 / channels)
        grad = jnp.concatenate(split3(grad)[:2], axis=0)
        spread = dot(wide_left, jnp.concatenate([grad, grad], axis=0), 1, 0)
        result = inv_ref[pl.ds(j, 1), :] * (spread - unit_ref[j, part, :].astype(F32) * joint)
        out_ref[pl.ds(pl.multiple_of(j * own, own), own), :] = result.astype(BF)
        return carry

    high, middle = left[:, :heads], left[:, heads : 2 * heads]
    wide_left = jnp.concatenate([high, high, middle, middle], axis=1)
    lax.fori_loop(0, keys, one, 0, unroll=UNROLL)


def weight_body(sizes, index_ref, *refs):
    samp, row, col = sizes
    blocks = samp * row
    factors = refs[:blocks]
    halves = refs[blocks : blocks + 2]
    in_out, out_out, left, normed, cot, sems = refs[blocks + 2 :]
    spot = Spot(index_ref, sizes)
    rows = factors[0].shape[1]
    width = normed.shape[1]
    slab = rows // col
    inner = out_out.shape[0]
    copies = []
    for q in range(row):
        for t in range(samp):
            place = lax.rem(spot.samp - t + samp, samp) * row + lax.rem(spot.row - q + row, row)
            begin = pl.multiple_of(place * rows, rows)
            copies.append((factors[q * samp + t], left.at[:, pl.ds(begin, rows)]))
            place = (spot.samp ^ t) * row + (spot.row ^ q)
            for k in range(col):
                source = halves[k % 2]
                begin = pl.multiple_of(place * rows + (spot.col ^ k) * slab, slab)
                rows_of = pl.ds((((k // 2) * row + q) * samp + t) * slab, slab)
                target = pl.ds(begin, slab)
                copies.append((source.at[rows_of, pl.ds(0, width)], normed.at[target, :]))
                copies.append((source.at[rows_of, pl.ds(width, width)], cot.at[target, :]))
    running = [
        pltpu.make_async_copy(source, target, sems.at[k])
        for k, (source, target) in enumerate(copies)
    ]
    for copy in running:
        copy.start()
    for copy in running:
        copy.wait()
    out_out[...] = dot(left[:inner], cot[...], 1, 0).astype(BF)
    for m in range(in_out.shape[0] // inner):
        part = slice(m * inner, (m + 1) * inner)
        in_out[part] = dot(left[(m + 1) * inner : (m + 2) * inner], normed[...], 1, 0).astype(BF)


def vmem(count):
    return [pl.BlockSpec(memory_space=pltpu.VMEM)] * count


SCALARS = pl.BlockSpec(memory_space=pltpu.SMEM)


def call(body, outs, specs, scratch=(), flops=1 << 20):
    return pl.pallas_call(
        body,
        out_shape=[jax.ShapeDtypeStruct(shape, kind) for shape, kind in outs],
        in_specs=specs,
        out_specs=vmem(len(outs)),
        scratch_shapes=list(scratch),
        compiler_params=pltpu.CompilerParams(vmem_limit_bytes=58 * 1024 * 1024),
        cost_estimate=pl.CostEstimate(flops=flops, bytes_accessed=1 << 20, transcendentals=0),
    )


def shifted(array, axis, step):
    size = lax.axis_size(axis)
    return lax.ppermute(array, axis, [(i, (i + step) % size) for i in range(size)])


def add(first, second):
    return (first.astype(F32) + second.astype(F32)).astype(BF)


def swapped(array, axis, mask):
    size = lax.axis_size(axis)
    return lax.ppermute(array, axis, [(i, i ^ mask) for i in range(size)])


def on_device(
    tokens,
    atom_type,
    noise_step,
    pair_rep,
    bond_blocks,
    chiral_blocks,
    type_table,
    noise_row,
    norm_gain,
    pair_gain,
    in_weight,
    out_weight,
    pair_weight,
    restraint_weight,
    cotangent,
):
    sizes = tuple(lax.axis_size(axis) for axis in ("samp", "row", "col"))
    samp, row, col = sizes
    rows, width = tokens.shape[1:]
    keys, channels = pair_rep.shape[1:]
    heads = pair_weight.shape[1]
    head_local = heads // col
    inner = in_weight.shape[1]
    members = in_weight.shape[0]
    count = rows * row
    own = channels // samp
    slab = rows // col
    anywhere = pl.BlockSpec(memory_space=pl.ANY)
    index = lax.axis_index(("samp", "row", "col")).astype(jnp.int32).reshape(1)
    cot = cotangent.reshape(rows, width)
    gain = norm_gain.reshape(-1, 128)
    pair_row = pair_gain.reshape(1, channels)
    weight = pair_weight.T

    pair = call(
        functools.partial(pair_body, sizes),
        [((head_local * keys, rows), F32)] * col
        + [((keys, channels, rows), BF), ((keys, rows), F32)],
        [SCALARS] + vmem(3),
        [pltpu.VMEM((rows * keys, channels), F32)],
        flops=1 << 30,
    )(index, pair_rep.reshape(rows * keys, channels), pair_row, weight)
    planes, (unit, inv) = pair[:col], pair[col:]
    arrived = [planes[0]] + [shifted(planes[k], "col", k) for k in range(1, col)]

    query, key_value, gates, piece, base = call(
        functools.partial(token_body, sizes),
        [
            ((inner, rows), BF),
            ((2 * inner, rows), BF),
            ((2 * inner, rows), F32),
            ((slab, 2 * width), BF),
            ((rows, width), F32),
        ],
        [SCALARS, SCALARS] + vmem(8) + [anywhere],
        [pltpu.VMEM((rows, width), BF)],
        flops=1 << 29,
    )(
        index,
        noise_step,
        tokens.reshape(rows, width),
        atom_type.reshape(1, rows),
        type_table,
        noise_row.reshape(-1, 128),
        gain,
        in_weight,
        out_weight,
        cot,
        inv,
    )
    key_values = [key_value] + [shifted(key_value, "row", t) for t in range(1, row)]

    early = piece
    for axis, size in (("samp", samp), ("row", row), ("col", col)):
        mask = 1 if axis != "col" else 2
        while mask < size:
            early = jnp.concatenate([early, swapped(early, axis, mask)], axis=0)
            mask *= 2
    halves = [early, swapped(early, "col", 1)]

    attention = call(
        functools.partial(attention_body, sizes, head_local),
        [((inner, rows), BF), ((2 * inner, rows), F32), ((2 * inner, rows), F32)]
        + [((2 * inner, rows), BF)] * (row - 1)
        + [((head_local * keys, rows), BF)] * col,
        [SCALARS, SCALARS] + vmem(4 + row + col),
        [
            pltpu.VMEM((inner, count), BF),
            pltpu.VMEM((inner, count), BF),
            pltpu.VMEM((head_local * count, rows), F32),
            pltpu.VMEM((2 * inner, count), F32),
            pltpu.VMEM((head_local * count, rows), BF),
        ],
        flops=1 << 29,
    )(index, restraint_weight, bond_blocks.T, chiral_blocks.T, query, gates, *key_values, *arrived)
    mixed, grads, own_kv = attention[:3]
    sends = attention[3 : 2 + row]
    bias_parts = attention[2 + row :]
    received = [shifted(sends[t - 1], "row", t) for t in range(1, row)]

    crossed = jnp.concatenate(
        [bias_parts[0]] + [shifted(bias_parts[k], "col", -k) for k in range(1, col)], axis=0
    )
    bias_sum = crossed
    mask = 1
    while 2 * mask < samp:
        bias_sum = add(bias_sum, swapped(bias_sum, "samp", mask))
        mask *= 2
    bias_other = swapped(bias_sum, "samp", mask)
    (proj,) = call(
        functools.partial(proj_body, sizes),
        [((heads, channels), F32)],
        [SCALARS] + vmem(3),
        [pltpu.VMEM((heads * keys, rows), F32)],
        flops=1 << 28,
    )(index, unit, pair_row, crossed)
    for axis, size in (("col", col), ("row", row), ("samp", samp)):
        mask = 1
        while mask < size:
            proj = proj + swapped(proj, axis, mask)
            mask *= 2

    factor, both = call(
        functools.partial(back_body, sizes),
        [(((1 + members) * inner, rows), BF), ((2 * rows, width), BF)],
        vmem(5 + row - 1),
        flops=1 << 29,
    )(grads, own_kv, mixed, in_weight.reshape(members * inner, width), out_weight, *received)
    factors = [factor] + [shifted(factor, "samp", t) for t in range(1, samp)]
    for q in range(1, row):
        factors += [shifted(one, "row", q) for one in factors[:samp]]
    mask = 1
    while 2 * mask < col:
        both = add(both, swapped(both, "col", mask))
        mask *= 2
    updated, token_grad = call(
        finish_body, [((rows, width), BF)] * 2, vmem(5), flops=1 << 28
    )(base, cot, gain, both, swapped(both, "col", mask))

    (pair_grad,) = call(
        functools.partial(pair_back_body, sizes),
        [((keys * own, rows), BF)],
        [SCALARS] + vmem(6 + col),
        [pltpu.VMEM((heads * keys, rows), F32)],
        flops=1 << 29,
    )(index, unit, inv, weight, pair_row, bias_sum, bias_other, *planes)

    blocks = samp * row
    hbm = pl.BlockSpec(memory_space=pltpu.HBM)
    in_grad, out_grad = call(
        functools.partial(weight_body, sizes),
        [((members * inner, width), BF), ((inner, width), BF)],
        [SCALARS] + [hbm] * (blocks + 2),
        [
            pltpu.VMEM(((1 + members) * inner, blocks * rows), BF),
            pltpu.VMEM((blocks * rows, width), BF),
            pltpu.VMEM((blocks * rows, width), BF),
            pltpu.SemaphoreType.DMA(((1 + 2 * col) * blocks,)),
        ],
        flops=1 << 30,
    )(index, *factors, *halves)
    return (
        updated.reshape(1, rows, width),
        token_grad.reshape(1, rows, width),
        pair_grad.reshape(keys, own, rows).transpose(2, 0, 1),
        in_grad.reshape(members, inner, width),
        out_grad,
        proj.T,
    )


def solution(mesh):
    placed = (
        P("samp", "row", None),
        P("row"),
        P("samp"),
        P("row", "col", None),
        P(),
        P(),
        P(),
        P(),
        P(),
        P(),
        P(None, "col", None),
        P("col", None),
        P(),
        P(),
        P("samp", "row", None),
    )
    return jax.shard_map(
        on_device,
        mesh=mesh,
        in_specs=placed,
        out_specs=(
            P("samp", "row", None),
            P("samp", "row", None),
            P("row", "col", "samp"),
            P(None, "col", None),
            P("col", None),
            P(),
        ),
        check_vma=False,
    )
```
